256 devices in a mesh: seq: 64 (over z, y, x_hi), tp: 4 (over x_lo, core).
Axes of the slice: x: 4 (x_hi: 2, x_lo: 2; x = x_hi * 2 + x_lo), y: 4, z: 8, core: 2. Of those that a mesh axis runs over, the one named last changes fastest.
Arguments:
- tokens: bfloat16 [32768, 2048], P('seq'), may hold values from -16 to 16
- forget: float32 [32768, 32], P('seq', 'tp'), may hold values from -5 to 0, as said below
- attn_gain: float32 [2048], replicated, may hold values from 0.1 to 1.9
- projections: bfloat16 [3, 2048, 2048], P(None, None, 'tp'), may hold values from -0.125 to 0.125
- out_weight: bfloat16 [2048, 2048], P('tp'), may hold values from -0.125 to 0.125
- ffn_gain: float32 [2048], replicated, may hold values from 0.1 to 1.9
- expand_weight: bfloat16 [2, 2048, 4096], P(None, None, 'tp'), may hold values from -0.125 to 0.125
- down_weight: bfloat16 [4096, 2048], P('tp'), may hold values from -0.09375 to 0.09375
Outputs:
- output: bfloat16 [32768, 2048], P('seq')
The draws below stay inside these ranges and needn't reach their ends.
Inputs may be any that keep to these rules, and one draw needn't show every extreme that they name: forget is never positive.
All inputs are finite; a program needn't handle non-finite values.
Results may differ from the reference program's by a relative error of at most 0.011.
Values may be sent and summed in bfloat16 or wider, within the bound.
A program may use at most 128 MiB of HBM per device.

```python
import math
import jax
import jax.numpy as jnp
from jax import lax

D = 2048
HEAD_TOTAL = 32
DH = 64
FF = 4096
TOK_DEV = 512
SEQUENCE_TOKENS = 32768


def draw_tokens(key, part):
    random_keys = jax.random.split(key, 3)
    noise = jax.random.normal(random_keys[0], (SEQUENCE_TOKENS, D), jnp.float32)
    row_scale = jnp.exp(jax.random.uniform(random_keys[1], (SEQUENCE_TOKENS, 1), jnp.float32, jnp.log(0.3), jnp.log(3.0)))
    column_scale = jnp.exp(jax.random.uniform(random_keys[2], (1, D), jnp.float32, jnp.log(0.3), jnp.log(3.0)))
    return jnp.clip(noise * row_scale * column_scale, -16.0, 16.0).astype(jnp.bfloat16)


def draw_forget(key, part):
    random_keys = jax.random.split(key, 7)
    slow_share = 0.5
    is_slow = jax.random.uniform(random_keys[0], (HEAD_TOTAL,), jnp.float32) < slow_share
    slow_rate = jax.random.uniform(random_keys[1], (HEAD_TOTAL,), jnp.float32, 0.2, 0.6) / SEQUENCE_TOKENS
    fast_rate = jnp.exp(jax.random.uniform(random_keys[2], (HEAD_TOTAL,), jnp.float32, jnp.log(10.0), jnp.log(16.0))) / TOK_DEV
    base_rate = jnp.where(is_slow, slow_rate, fast_rate)
    block_count = SEQUENCE_TOKENS // TOK_DEV
    device_factor = jnp.exp(jax.random.uniform(random_keys[3], (block_count, 1, HEAD_TOTAL), jnp.float32, jnp.log(0.5), jnp.log(2.0)))
    roughness = jax.random.uniform(random_keys[4], (block_count, TOK_DEV, HEAD_TOTAL), jnp.float32, 0.5, 1.5)
    decay_rates = (base_rate * device_factor * roughness).reshape(SEQUENCE_TOKENS, HEAD_TOTAL)
    spike_positions = jax.random.randint(random_keys[5], (2,), 0, SEQUENCE_TOKENS)
    spike_magnitude = jax.random.uniform(random_keys[6], (2, HEAD_TOTAL), jnp.float32, 0.22, 0.69)
    spike_flags = (jnp.arange(SEQUENCE_TOKENS)[:, None] == spike_positions[None, :]).astype(jnp.float32)
    spike_values = jnp.dot(spike_flags, spike_magnitude)
    return -(decay_rates + spike_values)


def block_scale(key, extent, shards, least, top_value):
    factor_of, own = 1.0, jax.random.fold_in(key, 6)
    for axis_at, blocks in shards:
        draws = jnp.exp(jax.random.uniform(jax.random.fold_in(own, axis_at), (blocks,), jnp.float32, least / len(shards), top_value / len(shards)))
        factor_of = factor_of * jnp.repeat(draws, extent[axis_at] // blocks).reshape([-1 if axis == axis_at else 1 for axis in range(len(extent))])
    return factor_of


def gaussian(stream_key, shape, width, reach, shards=(), dtype=jnp.bfloat16):
    entries = width * jax.random.normal(stream_key, shape, jnp.float32)
    if shards:
        entries = entries * block_scale(stream_key, shape, shards, -0.22, 0.18)
    return jnp.clip(entries, -reach, reach).astype(dtype)


def setup_inputs(seed: int = 0) -> dict:
    splits = jax.random.split(jax.random.key(seed), 9)
    tokens = draw_tokens(jax.random.fold_in(splits[8], 71), 0)
    forget = draw_forget(jax.random.fold_in(splits[8], 71), 0)
    attn_gain = jnp.clip(1.0 + 0.18 * jax.random.normal(splits[2], (D,), jnp.float32), 0.1, 1.9)
    projections = gaussian(splits[3], (3, D, HEAD_TOTAL * DH), D ** -0.5, 0.125, ((2, 4),))
    out_weight = gaussian(splits[4], (HEAD_TOTAL * DH, D), (HEAD_TOTAL * DH) ** -0.5, 0.125, ((0, 4),))
    ffn_gain = jnp.clip(1.0 + 0.18 * jax.random.normal(splits[5], (D,), jnp.float32), 0.1, 1.9)
    expand_weight = gaussian(splits[6], (2, D, FF), D ** -0.5, 0.125, ((2, 4),))
    down_weight = gaussian(splits[7], (FF, D), FF ** -0.5, 0.09375, ((0, 4),))
    return dict(tokens=tokens, forget=forget, attn_gain=attn_gain, projections=projections, out_weight=out_weight, ffn_gain=ffn_gain, expand_weight=expand_weight, down_weight=down_weight)


norm_epsilon = 1e-05
head_epsilon = 1e-06

def rms_scale(values, gain_vector):
    widened = values.astype(jnp.float32)
    mean_square = lax.optimization_barrier(jnp.mean(widened * widened, axis=-1, keepdims=True))
    return widened * lax.rsqrt(mean_square + norm_epsilon) * gain_vector

def summarize(key_rows, value_rows, forget_rows):
    log_decay = jnp.cumsum(forget_rows, axis=0)
    block_total = log_decay[-1]
    shrink_factors = jnp.exp(block_total[None, :] - log_decay)
    scaled_keys = (key_rows.astype(jnp.float32) * shrink_factors[:, :, None]).astype(jnp.bfloat16)
    block_state = jnp.einsum('shd,she->hde', scaled_keys.astype(jnp.float32), value_rows.astype(jnp.float32), precision=lax.Precision.HIGHEST)
    return (log_decay, block_total, block_state)

def attend_local(query_rows, key_rows, value_rows, log_decay, incoming):
    head_size = query_rows.shape[2]
    score_scale = 1.0 / math.sqrt(head_size)
    query_wide = query_rows.astype(jnp.float32)
    scores = jnp.einsum('thd,shd->hts', query_wide, key_rows.astype(jnp.float32), precision=lax.Precision.HIGHEST) * score_scale
    log_gaps = log_decay.T[:, :, None] - log_decay.T[:, None, :]
    row_order = jnp.arange(query_rows.shape[0])
    causal = (row_order[:, None] >= row_order[None, :])[None]
    local_weights = jnp.where(causal, scores * jnp.exp(jnp.where(causal, log_gaps, 0.0)), 0.0).astype(jnp.bfloat16)
    local_part = jnp.einsum('hts,she->the', local_weights.astype(jnp.float32), value_rows.astype(jnp.float32), precision=lax.Precision.HIGHEST)
    carried = jnp.einsum('thd,hde->the', query_wide, incoming, precision=lax.Precision.HIGHEST)
    attended = local_part + carried * (jnp.exp(log_decay) * score_scale)[:, :, None]
    mean_square = lax.optimization_barrier(jnp.mean(attended * attended, axis=-1, keepdims=True))
    return (attended * lax.rsqrt(mean_square + head_epsilon)).astype(jnp.bfloat16)

def reference(tokens, forget, attn_gain, projections, out_weight, ffn_gain, expand_weight, down_weight):
    normed = rms_scale(tokens, attn_gain).astype(jnp.bfloat16)
    block_count = SEQUENCE_TOKENS // TOK_DEV
    shaped = []
    for which in range(3):
        projected = jnp.dot(normed, projections[which], preferred_element_type=jnp.float32).astype(jnp.bfloat16)
        shaped.append(projected.reshape(block_count, TOK_DEV, HEAD_TOTAL, DH))
    forget_blocks = forget.reshape(block_count, TOK_DEV, HEAD_TOTAL)

    def block_step(incoming, block_data):
        query_rows, key_rows, value_rows, forget_rows = block_data
        log_decay, block_total, block_state = summarize(key_rows, value_rows, forget_rows)
        head_out = attend_local(query_rows, key_rows, value_rows, log_decay, incoming)
        following = jnp.exp(block_total)[:, None, None] * incoming + block_state
        return (following, head_out)
    start_state = jnp.zeros((HEAD_TOTAL, DH, DH), jnp.float32)
    _, head_blocks = lax.scan(block_step, start_state, (shaped[0], shaped[1], shaped[2], forget_blocks))
    head_out = head_blocks.reshape(SEQUENCE_TOKENS, HEAD_TOTAL * DH)
    attn_out = jnp.dot(head_out, out_weight, preferred_element_type=jnp.float32)
    residual = (tokens.astype(jnp.float32) + attn_out).astype(jnp.bfloat16)
    normed_ffn = rms_scale(residual, ffn_gain).astype(jnp.bfloat16)
    gate_proj = jnp.dot(normed_ffn, expand_weight[0], preferred_element_type=jnp.float32)
    up_proj = jnp.dot(normed_ffn, expand_weight[1], preferred_element_type=jnp.float32)
    hidden = (jax.nn.silu(gate_proj) * up_proj).astype(jnp.bfloat16)
    ffn_out = jnp.dot(hidden, down_weight, preferred_element_type=jnp.float32)
    return (residual.astype(jnp.float32) + ffn_out).astype(jnp.bfloat16)
```

```python
import functools

import jax
import jax.numpy as jnp
from jax import lax
from jax.experimental import pallas as pl
from jax.experimental.pallas import tpu as pltpu
from jax.sharding import PartitionSpec as P

MESH = pl.DeviceIdType.MESH
F32 = jnp.float32
BF16 = jnp.bfloat16

norm_epsilon = 1e-05
head_epsilon = 1e-06

TOK = 512
D = 2048
HD = 512
FF = 1024
CH = 4
RW = TOK // CH
OW = RW // 4
NP = 4
PLANE = 8
DEPTH = 8


def dot(a, b):
    return jnp.dot(a, b, preferred_element_type=F32)


def kernel(
    tok_h, forget_h, again_h, proj_h, outw_h, fgain_h, exp_h, down_h, out_h,
    tok, fgt, again, fgain, proj, outw, wexp, wdown,
    normed, qs, ks, vs, ld, ldt, ldx, local,
    ldsend, ld_in, ltsend, lt_in, ssend, s_in, pref, tsend, t_in, isend, i_in, inc,
    ho, psend, prec, pk, pisend, pirec,
    resid, xrows, hidden, ysend, yrec, yk, yisend, yirec, out,
    tok_sem, w_sem, out_sem,
    ld_ss, ld_rs, lt_ss, lt_rs, s_ss, s_rs, t_ss, t_rs, i_ss, i_rs,
    p_ss, p_rs, pi_ss, pi_rs, xd_ss, xd_rs, xi_ss, xi_rs, xf_ss, xf_rs,
    y_ss, y_rs, yi_ss, yi_rs, od_ss, od_rs, oi_ss, oi_rs, of_ss, of_rs,
):
    s = lax.axis_index("seq")
    t = lax.axis_index("tp")
    plane = lax.rem(s, PLANE)
    z = s // PLANE
    c = t // 2
    k = lax.rem(t, 2)
    core_peer = (s, c * 2 + (1 - k))
    chip_peer = (s, (1 - c) * 2 + k)
    ffn_peer = (s + 1 - 2 * lax.rem(s, 2), (1 - c) * 2 + k)

    def plane_peer(d):
        j = lax.rem(plane + d, PLANE)
        return j, (z * PLANE + j, t)

    def depth_peer(d):
        j = lax.rem(z + d, DEPTH)
        return j, (j * PLANE + plane, t)

    def remote(src, dst, ssem, rsem, dev):
        return pltpu.make_async_remote_copy(
            src_ref=src, dst_ref=dst, send_sem=ssem, recv_sem=rsem,
            device_id=dev, device_id_type=MESH,
        )

    barrier = pltpu.get_barrier_semaphore()
    for d in range(1, PLANE):
        pl.semaphore_signal(barrier, inc=1, device_id=plane_peer(d)[1], device_id_type=MESH)
    for d in range(1, DEPTH):
        pl.semaphore_signal(barrier, inc=1, device_id=depth_peer(d)[1], device_id_type=MESH)
    for dev in (core_peer, chip_peer, ffn_peer):
        pl.semaphore_signal(barrier, inc=1, device_id=dev, device_id_type=MESH)

    def tok_copy(i):
        rows = pl.ds(i * RW, RW)
        return pltpu.make_async_copy(tok_h.at[rows], tok.at[rows], tok_sem.at[i])

    for i in range(CH):
        tok_copy(i).start()
    forget_copy = pltpu.make_async_copy(forget_h, fgt, w_sem.at[0])
    again_copy = pltpu.make_async_copy(again_h, again, w_sem.at[1])
    proj_copies = [
        pltpu.make_async_copy(proj_h.at[w], proj.at[w], w_sem.at[2 + w]) for w in range(3)
    ]
    fgain_copy = pltpu.make_async_copy(fgain_h, fgain, w_sem.at[5])
    outw_copy = pltpu.make_async_copy(outw_h, outw, w_sem.at[6])
    exp_copy = pltpu.make_async_copy(exp_h, wexp, w_sem.at[7])
    down_copy = pltpu.make_async_copy(down_h, wdown, w_sem.at[8])
    forget_copy.start()
    again_copy.start()
    proj_copies[1].start()
    proj_copies[2].start()

    forget_copy.wait()
    f = fgt[...]
    f1 = f.astype(BF16)
    rest = f - f1.astype(F32)
    f2 = rest.astype(BF16)
    f3 = (rest - f2.astype(F32)).astype(BF16)
    row_at = lax.broadcasted_iota(jnp.int32, (TOK, TOK), 0)
    col_at = lax.broadcasted_iota(jnp.int32, (TOK, TOK), 1)
    lower = jnp.where(row_at >= col_at, 1.0, 0.0).astype(BF16)
    sums = dot(lower, f1) + (dot(lower, f2) + dot(lower, f3))
    ld[:, 0:8] = sums
    ld[:, 8:128] = jnp.zeros((TOK, 120), F32)
    turned = jnp.transpose(ld[...])
    for h in range(8):
        ldt[h] = turned[h : h + 1]
    total = jnp.broadcast_to(turned[0:8, TOK - 1 : TOK], (8, 128))
    ldsend[...] = total
    ld_in[plane] = total

    low_lanes = lax.broadcasted_iota(jnp.int32, (RW, 128), 1) < 64
    for i in range(CH):
        for p in range(NP):
            rows = slice(i * RW, (i + 1) * RW)
            ldx[rows, p * 128 : (p + 1) * 128] = jnp.where(
                low_lanes, ld[rows, 2 * p : 2 * p + 1], ld[rows, 2 * p + 1 : 2 * p + 2]
            )

    again_copy.wait()

    def norm_rows(i, _):
        pltpu.make_async_copy(
            tok_h.at[pl.ds(i * RW, RW)], tok.at[pl.ds(i * RW, RW)], tok_sem.at[i]
        ).wait()
        rows = pl.ds(pl.multiple_of(i * RW, RW), RW)
        x = tok[rows, :].astype(F32)
        mean_square = jnp.sum(x * x, axis=1, keepdims=True) * (1.0 / D)
        scale = lax.rsqrt(mean_square + norm_epsilon)
        normed[rows, :] = (tok[rows, :].astype(F32) * scale * again[...]).astype(BF16)
        return _

    lax.fori_loop(0, CH, norm_rows, 0)

    proj_copies[0].start()
    fgain_copy.start()
    outw_copy.start()
    exp_copy.start()
    down_copy.start()

    pl.semaphore_wait(barrier, PLANE - 1 + DEPTH - 1 + 3)
    for d in range(1, PLANE):
        j, dev = plane_peer(d)
        remote(ldsend, ld_in.at[plane], ld_ss.at[d], ld_rs.at[d], dev).start()

    proj_copies[1].wait()
    ks[...] = dot(normed[...], proj[1]).astype(BF16)
    proj_copies[2].wait()
    vs[...] = dot(normed[...], proj[2]).astype(BF16)

    lanes32 = lax.broadcasted_iota(jnp.int32, (32, 128), 1) < 64
    for p in range(NP):
        cols = slice(p * 128, (p + 1) * 128)
        decay = jnp.exp(ldx[TOK - 1 : TOK, cols] - ldx[:, cols])
        scaled = (ks[:, cols].astype(F32) * decay).astype(BF16)
        m = lax.dot_general(
            scaled, vs[:, cols], (((0,), (0,)), ((), ())), preferred_element_type=F32
        )
        even = jnp.where(lanes32, m[0:32], pltpu.roll(m[32:64], 64, 1))
        odd = jnp.where(lanes32, pltpu.roll(m[64:96], 64, 1), m[96:128])
        ssend[2 * p] = even.astype(BF16)
        ssend[2 * p + 1] = odd.astype(BF16)

    s_in[plane] = ssend[plane]
    for d in range(1, PLANE):
        j, dev = plane_peer(d)
        remote(ssend.at[j], s_in.at[plane], s_ss.at[d], s_rs.at[d], dev).start()

    for d in range(1, PLANE):
        remote(ldsend, ld_in.at[0], ld_ss.at[d], ld_rs.at[d], core_peer).wait_recv()
    plane_total = ld_in[0]
    for j in range(1, PLANE):
        plane_total = plane_total + ld_in[j]
    ltsend[...] = plane_total
    lt_in[z] = plane_total
    for d in range(1, DEPTH):
        j, dev = depth_peer(d)
        remote(ltsend, lt_in.at[z], lt_ss.at[d], lt_rs.at[d], dev).start()

    proj_copies[0].wait()
    qs[...] = (dot(normed[...], proj[0]) * 0.125).astype(BF16)

    def send_totals():
        for d in range(1, PLANE):
            remote(ssend.at[0], s_in.at[0], s_ss.at[d], s_rs.at[d], core_peer).wait_recv()
        state = jnp.zeros((32, 128), F32)
        for j in range(PLANE):
            pref[j] = state
            state = jnp.exp(ld_in[j, pl.ds(plane, 1), :]) * state + s_in[j].astype(F32)
        rounded = state.astype(BF16)
        tsend[...] = rounded
        t_in[z] = rounded
        for d in range(1, DEPTH):
            j, dev = depth_peer(d)
            remote(tsend, t_in.at[z], t_ss.at[d], t_rs.at[d], dev).start()

    def send_prefixes():
        for d in range(1, DEPTH):
            remote(ltsend, lt_in.at[0], lt_ss.at[d], lt_rs.at[d], core_peer).wait_recv()
            remote(tsend, t_in.at[0], t_ss.at[d], t_rs.at[d], core_peer).wait_recv()
        state = jnp.zeros((32, 128), F32)
        for j in range(DEPTH):
            following = jnp.exp(lt_in[j, pl.ds(plane, 1), :]) * state + t_in[j].astype(F32)
            state = jnp.where(j < z, following, state)
        passed = jnp.zeros((1, 128), F32)
        for j in range(PLANE):
            isend[j] = (pref[j] + jnp.exp(passed) * state).astype(BF16)
            passed = passed + ld_in[j, pl.ds(plane, 1), :]
        i_in[plane] = isend[plane]
        for d in range(1, PLANE):
            j, dev = plane_peer(d)
            remote(isend.at[j], i_in.at[plane], i_ss.at[d], i_rs.at[d], dev).start()

    lanes512 = lax.broadcasted_iota(jnp.int32, (TOK, 128), 1) < 64
    causal = lax.broadcasted_iota(jnp.int32, (RW, RW), 0) >= lax.broadcasted_iota(
        jnp.int32, (RW, RW), 1
    )
    zero = jnp.zeros((), BF16)

    def pair_step(p, _):
        cols = pl.ds(pl.multiple_of(p * 128, 128), 128)
        kp = ks[:, cols]
        vp = vs[:, cols]
        for h in range(2):
            mine = lanes512 if h == 0 else jnp.logical_not(lanes512)
            vh = jnp.where(mine, vp.astype(F32), 0.0).astype(BF16)
            for i in range(CH):
                rows = slice(i * RW, (i + 1) * RW)
                span = (i + 1) * RW
                qh = jnp.where(mine[0:RW], qs[rows, cols].astype(F32), 0.0).astype(BF16)
                scores = lax.dot_general(
                    qh, kp[0:span], (((1,), (1,)), ((), ())), preferred_element_type=F32
                )
                here = ldx[rows, cols][:, 64 * h : 64 * h + 1]
                there = ldt[2 * p + h]
                parts = []
                for b in range(i + 1):
                    gap = here - there[:, b * RW : (b + 1) * RW]
                    if b == i:
                        gap = jnp.where(causal, gap, -1e30)
                    parts.append(
                        (scores[:, b * RW : (b + 1) * RW] * jnp.exp(gap)).astype(BF16)
                    )
                weights = parts[0] if i == 0 else jnp.concatenate(parts, axis=1)
                part = dot(weights, vh[0:span])
                if h == 0:
                    local[rows, cols] = part
                else:
                    local[rows, cols] = local[rows, cols] + part

        @pl.when(p == 1)
        def _totals():
            send_totals()

        @pl.when(p == 3)
        def _prefixes():
            send_prefixes()

        return _

    lax.fori_loop(0, NP, pair_step, 0)

    for d in range(1, PLANE):
        remote(isend.at[0], i_in.at[0], i_ss.at[d], i_rs.at[d], core_peer).wait_recv()
    for p in range(NP):
        even = i_in[2 * p].astype(F32)
        odd = i_in[2 * p + 1].astype(F32)
        inc[p, 0:32, :] = jnp.where(lanes32, even, 0.0).astype(BF16)
        inc[p, 32:64, :] = jnp.where(lanes32, pltpu.roll(even, 64, 1), 0.0).astype(BF16)
        inc[p, 64:96, :] = jnp.where(lanes32, 0.0, pltpu.roll(odd, 64, 1)).astype(BF16)
        inc[p, 96:128, :] = jnp.where(lanes32, 0.0, odd).astype(BF16)

    same_head = jnp.where(
        (lax.broadcasted_iota(jnp.int32, (128, 128), 0) < 64)
        == (lax.broadcasted_iota(jnp.int32, (128, 128), 1) < 64),
        1.0,
        0.0,
    ).astype(BF16)

    def partial_to_core(i):
        return remote(psend.at[i], prec.at[i], p_ss.at[i], p_rs.at[i], core_peer)

    def partial_to_chip(i):
        return remote(pisend.at[i], pirec.at[i], pi_ss.at[i], pi_rs.at[i], chip_peer)

    def stage_a(i):
        rows = pl.ds(pl.multiple_of(i * RW, RW), RW)
        for p in range(NP):
            cols = slice(p * 128, (p + 1) * 128)
            carried = dot(qs[rows, cols], inc[p])
            attended = local[rows, cols] + carried * jnp.exp(ldx[rows, cols])
            square = attended * attended
            high = square.astype(BF16)
            low = (square - high.astype(F32)).astype(BF16)
            mean_square = (dot(high, same_head) + dot(low, same_head)) * (1.0 / 64)
            headed = (attended * lax.rsqrt(mean_square + head_epsilon)).astype(BF16)
            for kk in range(2):
                core_slot = 1 - k if kk == 0 else k
                for cc in range(2):
                    chip_slot = c if cc == 0 else 1 - c
                    at = pl.multiple_of(core_slot * 2 * OW + chip_slot * OW, OW)
                    ho[pl.ds(at, OW), cols] = headed[(kk * 2 + cc) * OW : (kk * 2 + cc + 1) * OW]
        for n in range(4):
            cols = slice(n * 512, (n + 1) * 512)
            part = dot(ho[...], outw[:, cols])
            psend[i, :, cols] = part[0 : 2 * OW].astype(BF16)
            pk[i, :, cols] = part[2 * OW : 4 * OW]
        partial_to_core(i).start()

    def stage_b(i):
        partial_to_core(i).wait_recv()
        pisend[i] = (pk[i, OW : 2 * OW, :] + prec[i, OW : 2 * OW, :].astype(F32)).astype(BF16)
        partial_to_chip(i).start()

    own_at = k * 2 * OW + c * OW

    def rows_to_core(i):
        return remote(
            xrows.at[i, pl.ds(2 * OW, OW)], xrows.at[i, pl.ds(0, OW)],
            xd_ss.at[i], xd_rs.at[i], core_peer,
        )

    def rows_to_ffn(i):
        return remote(
            xrows.at[i, pl.ds(2 * OW, OW)], xrows.at[i, pl.ds(3 * OW, OW)],
            xi_ss.at[i], xi_rs.at[i], ffn_peer,
        )

    def rows_forward(i):
        return remote(
            xrows.at[i, pl.ds(3 * OW, OW)], xrows.at[i, pl.ds(OW, OW)],
            xf_ss.at[i], xf_rs.at[i], core_peer,
        )

    def stage_c(i):
        partial_to_chip(i).wait_recv()
        rows = pl.ds(pl.multiple_of(i * RW + own_at, OW), OW)
        res = (
            tok[rows, :].astype(F32)
            + (pk[i, 0:OW, :] + prec[i, 0:OW, :].astype(F32) + pirec[i].astype(F32))
        ).astype(BF16)
        resid[i] = res
        wide = res.astype(F32)
        mean_square = jnp.sum(wide * wide, axis=1, keepdims=True) * (1.0 / D)
        scale = lax.rsqrt(mean_square + norm_epsilon)
        xrows[i, 2 * OW : 3 * OW, :] = (wide * scale * fgain[...]).astype(BF16)
        rows_to_ffn(i).start()
        rows_to_core(i).start()

    def stage_d(i):
        rows_to_ffn(i).wait_recv()
        rows_forward(i).start()

    def sums_to_core(i):
        return remote(ysend.at[i], yrec.at[i], y_ss.at[i], y_rs.at[i], core_peer)

    def sums_to_ffn(i):
        return remote(yisend.at[i], yirec.at[i], yi_ss.at[i], yi_rs.at[i], ffn_peer)

    def stage_e_expand(i):
        rows_to_core(i).wait_recv()
        rows_forward(i).wait_recv()
        x = xrows.at[i]
        for n in range(4):
            cols = slice(n * 256, (n + 1) * 256)
            gate = dot(x[...], wexp[0, :, cols])
            up = dot(x[...], wexp[1, :, cols])
            hidden[:, cols] = (gate / (1.0 + jnp.exp(-gate)) * up).astype(BF16)

    def stage_e_down(i):
        for n in range(4):
            cols = slice(n * 512, (n + 1) * 512)
            part = dot(hidden[...], wdown[:, cols])
            ysend[i, :, cols] = part[0 : 2 * OW].astype(BF16)
            yk[i, :, cols] = part[2 * OW : 4 * OW]
        sums_to_core(i).start()

    def stage_f(i):
        sums_to_core(i).wait_recv()
        yisend[i] = (yk[i, OW : 2 * OW, :] + yrec[i, OW : 2 * OW, :].astype(F32)).astype(BF16)
        sums_to_ffn(i).start()

    own_rows = pl.ds(pl.multiple_of(own_at, OW), OW)
    chip_rows = pl.ds(pl.multiple_of(k * 2 * OW + (1 - c) * OW, OW), OW)

    def out_to_core(i):
        return remote(
            out.at[i, own_rows], out.at[i, own_rows], od_ss.at[i], od_rs.at[i], core_peer
        )

    def out_to_chip(i):
        return remote(
            out.at[i, own_rows], out.at[i, own_rows], oi_ss.at[i], oi_rs.at[i], chip_peer
        )

    def out_forward(i):
        return remote(
            out.at[i, chip_rows], out.at[i, chip_rows], of_ss.at[i], of_rs.at[i], core_peer
        )

    def stage_g(i):
        sums_to_ffn(i).wait_recv()
        out[i, own_rows, :] = (
            resid[i].astype(F32)
            + (yk[i, 0:OW, :] + yrec[i, 0:OW, :].astype(F32) + yirec[i].astype(F32))
        ).astype(BF16)
        out_to_chip(i).start()
        out_to_core(i).start()

    def stage_h(i):
        out_to_chip(i).wait_recv()
        out_forward(i).start()

    def out_copy(i):
        return pltpu.make_async_copy(out.at[i], out_h.at[pl.ds(i * RW, RW)], out_sem.at[i])

    def finish(i):
        out_to_core(i).wait_recv()
        out_forward(i).wait_recv()
        out_copy(i).start()

    outw_copy.wait()
    fgain_copy.wait()

    def heads_step(i, _):
        stage_a(i)

        @pl.when(i > 0)
        def _sum():
            stage_b(i - 1)

        return _

    lax.fori_loop(0, CH, heads_step, 0)
    stage_b(CH - 1)
    stage_c(0)
    stage_c(1)
    exp_copy.wait()
    down_copy.wait()
    stage_d(0)
    stage_c(2)

    def ffn_step(i, _):
        stage_e_expand(i)

        @pl.when(i == 0)
        def _rows():
            stage_c(3)

        @pl.when(i < CH - 1)
        def _forward():
            stage_d(i + 1)

        @pl.when(i > 0)
        def _sum():
            stage_f(i - 1)

        @pl.when(i == CH - 1)
        def _output():
            stage_g(0)

        stage_e_down(i)
        return _

    lax.fori_loop(0, CH, ffn_step, 0)
    stage_g(1)
    stage_f(3)
    stage_h(0)
    stage_g(2)
    stage_h(1)
    finish(0)
    stage_g(3)
    stage_h(2)
    finish(1)
    stage_h(3)
    finish(2)
    finish(3)

    for d in range(1, PLANE):
        remote(ldsend, ld_in.at[0], ld_ss.at[d], ld_rs.at[d], core_peer).wait_send()
        remote(ssend.at[0], s_in.at[0], s_ss.at[d], s_rs.at[d], core_peer).wait_send()
        remote(isend.at[0], i_in.at[0], i_ss.at[d], i_rs.at[d], core_peer).wait_send()
    for d in range(1, DEPTH):
        remote(ltsend, lt_in.at[0], lt_ss.at[d], lt_rs.at[d], core_peer).wait_send()
        remote(tsend, t_in.at[0], t_ss.at[d], t_rs.at[d], core_peer).wait_send()
    for i in range(CH):
        for copy in (
            partial_to_core, partial_to_chip, rows_to_core, rows_to_ffn, rows_forward,
            sums_to_core, sums_to_ffn, out_to_core, out_to_chip, out_forward,
        ):
            copy(i).wait_send()
        out_copy(i).wait()


def local_layer(tokens, forget, attn_gain, projections, out_weight, ffn_gain, expand_weight, down_weight):
    dma = pltpu.SemaphoreType.DMA
    vmem = pltpu.VMEM
    scratch = [
        vmem((TOK, D), BF16),
        vmem((TOK, 8), F32),
        vmem((1, D), F32),
        vmem((1, D), F32),
        vmem((3, D, HD), BF16),
        vmem((HD, D), BF16),
        vmem((2, D, FF), BF16),
        vmem((FF, D), BF16),
        vmem((TOK, D), BF16),
        vmem((TOK, HD), BF16),
        vmem((TOK, HD), BF16),
        vmem((TOK, HD), BF16),
        vmem((TOK, 128), F32),
        vmem((8, 1, TOK), F32),
        vmem((TOK, HD), F32),
        vmem((TOK, HD), F32),
        vmem((8, 128), F32),
        vmem((PLANE, 8, 128), F32),
        vmem((8, 128), F32),
        vmem((DEPTH, 8, 128), F32),
        vmem((PLANE, 32, 128), BF16),
        vmem((PLANE, 32, 128), BF16),
        vmem((PLANE, 32, 128), F32),
        vmem((32, 128), BF16),
        vmem((DEPTH, 32, 128), BF16),
        vmem((PLANE, 32, 128), BF16),
        vmem((PLANE, 32, 128), BF16),
        vmem((NP, 128, 128), BF16),
        vmem((RW, HD), BF16),
        vmem((CH, 2 * OW, D), BF16),
        vmem((CH, 2 * OW, D), BF16),
        vmem((CH, 2 * OW, D), F32),
        vmem((CH, OW, D), BF16),
        vmem((CH, OW, D), BF16),
        vmem((CH, OW, D), BF16),
        vmem((CH, RW, D), BF16),
        vmem((RW, FF), BF16),
        vmem((CH, 2 * OW, D), BF16),
        vmem((CH, 2 * OW, D), BF16),
        vmem((CH, 2 * OW, D), F32),
        vmem((CH, OW, D), BF16),
        vmem((CH, OW, D), BF16),
        vmem((CH, RW, D), BF16),
        dma((CH,)),
        dma((9,)),
        dma((CH,)),
    ]
    scratch += [dma((8,)) for _ in range(10)]
    scratch += [dma((CH,)) for _ in range(20)]
    any_spec = pl.BlockSpec(memory_space=pl.ANY)
    return pl.pallas_call(
        kernel,
        out_shape=jax.ShapeDtypeStruct((TOK, D), BF16),
        in_specs=[any_spec] * 8,
        out_specs=any_spec,
        scratch_shapes=scratch,
        name="layer",
        compiler_params=pltpu.CompilerParams(
            collective_id=0, has_side_effects=True, vmem_limit_bytes=62 * 1024 * 1024
        ),
    )(
        tokens,
        forget,
        attn_gain.reshape(1, D),
        projections,
        out_weight,
        ffn_gain.reshape(1, D),
        expand_weight,
        down_weight,
    )


def solution(mesh):
    return jax.shard_map(
        local_layer,
        mesh=mesh,
        in_specs=(
            P("seq", None),
            P("seq", "tp"),
            P(),
            P(None, None, "tp"),
            P("tp", None),
            P(),
            P(None, None, "tp"),
            P("tp", None),
        ),
        out_specs=P("seq", None),
        check_vma=False,
    )
```

```python
import functools

import jax
import jax.numpy as jnp
from jax import lax
from jax.experimental import pallas as pl
from jax.experimental.pallas import tpu as pltpu
from jax.sharding import PartitionSpec as P

MESH = pl.DeviceIdType.MESH
F32 = jnp.float32
BF16 = jnp.bfloat16

norm_epsilon = 1e-05
head_epsilon = 1e-06

TOK = 512
D = 2048
HD = 512
FF = 1024
CH = 8
EG = 2
HG = 2
AB = 128
RW = TOK // CH
OW = RW // 4
NP = 4
PLANE = 8
DEPTH = 8


ORDER = (
    "A0 A1 B0 B1", "B2 B3 A2 A3", "B5 C0 B4 B6", "C1 C2 C3 B7", "D0 C5 D1 C4", "D2 C6 X0 D3",
    "C7 Y0 D5 X1", "D4 F1 F0 Y1", "D6 X2 D7 F2", "F3 Y2 X3 F4", "G1 Y3 G0 F5", "F6 G2 F7 G3",
    "H1 G4 G5 G6", "G7 H2 H4 H5", "H3 Z4 H6 H0", "H7 Z1 Z3 Z5", "Z7 Z0 Z2 Z6",
)


def dot(a, b):
    return jnp.dot(a, b, preferred_element_type=F32)


def kernel(
    tok_h, forget_h, again_h, proj_h, outw_h, fgain_h, exp_h, down_h, out,
    tok, fgt, again, fgain, proj, outw, wexp, wdown,
    normed, qs, ks, vs, ld, ldt, ldx, local,
    ldsend, ld_in, ltsend, lt_in, ssend, s_in, pref, carry, tsend, t_in, isend, i_in, inc,
    ho, psend, prec, pk, pisend, pirec,
    resid, xrows, hidden, ysend, yrec, yk, yisend, yirec,
    tok_sem, w_sem,
    ld_ss, ld_rs, lt_ss, lt_rs, s_ss, s_rs, t_ss, t_rs, i_ss, i_rs,
    p_ss, p_rs, pi_ss, pi_rs, xd_ss, xd_rs, xi_ss, xi_rs, xf_ss, xf_rs,
    y_ss, y_rs, yi_ss, yi_rs, od_ss, od_rs, oi_ss, oi_rs, of_ss, of_rs,
):
    s = lax.axis_index("seq")
    t = lax.axis_index("tp")
    plane = lax.rem(s, PLANE)
    z = s // PLANE
    c = t // 2
    k = lax.rem(t, 2)
    core_peer = (s, c * 2 + (1 - k))
    chip_peer = (s, (1 - c) * 2 + k)
    ffn_peer = (s + 1 - 2 * lax.rem(s, 2), (1 - c) * 2 + k)

    def plane_peer(d):
        j = lax.rem(plane + d, PLANE)
        return j, (z * PLANE + j, t)

    def depth_peer(d):
        j = lax.rem(z + d, DEPTH)
        return j, (j * PLANE + plane, t)

    def remote(src, dst, ssem, rsem, dev):
        return pltpu.make_async_remote_copy(
            src_ref=src, dst_ref=dst, send_sem=ssem, recv_sem=rsem,
            device_id=dev, device_id_type=MESH,
        )

    barrier = pltpu.get_barrier_semaphore()
    for d in range(1, PLANE):
        pl.semaphore_signal(barrier, inc=1, device_id=plane_peer(d)[1], device_id_type=MESH)
    for d in range(1, DEPTH):
        pl.semaphore_signal(barrier, inc=1, device_id=depth_peer(d)[1], device_id_type=MESH)
    for dev in (core_peer, chip_peer, ffn_peer):
        pl.semaphore_signal(barrier, inc=1, device_id=dev, device_id_type=MESH)

    for i in range(TOK // AB):
        rows = pl.ds(i * AB, AB)
        pltpu.make_async_copy(tok_h.at[rows], tok.at[rows], tok_sem.at[i]).start()
    forget_copy = pltpu.make_async_copy(forget_h, fgt, w_sem.at[0])
    again_copy = pltpu.make_async_copy(again_h, again, w_sem.at[1])
    proj_copies = [
        pltpu.make_async_copy(proj_h.at[w], proj.at[w], w_sem.at[2 + w]) for w in range(3)
    ]
    fgain_copy = pltpu.make_async_copy(fgain_h, fgain, w_sem.at[5])
    outw_copy = pltpu.make_async_copy(outw_h, outw, w_sem.at[6])
    exp_copy = pltpu.make_async_copy(exp_h, wexp, w_sem.at[7])
    down_copy = pltpu.make_async_copy(down_h, wdown, w_sem.at[8])
    forget_copy.start()
    again_copy.start()
    proj_copies[1].start()
    proj_copies[2].start()

    forget_copy.wait()
    f = fgt[...]
    f1 = f.astype(BF16)
    rest = f - f1.astype(F32)
    f2 = rest.astype(BF16)
    f3 = (rest - f2.astype(F32)).astype(BF16)
    row_at = lax.broadcasted_iota(jnp.int32, (TOK, TOK), 0)
    col_at = lax.broadcasted_iota(jnp.int32, (TOK, TOK), 1)
    upper = jnp.where(row_at <= col_at, 1.0, 0.0).astype(BF16)
    turned = dot(f1, upper) + (dot(f2, upper) + dot(f3, upper))
    for h in range(8):
        ldt[h] = turned[h : h + 1]
    ld[...] = jnp.transpose(jnp.concatenate([turned, jnp.zeros((120, TOK), F32)], axis=0))
    total = jnp.broadcast_to(turned[:, TOK - 1 : TOK], (8, 128))
    for h in range(8):
        ldsend[h] = total[h : h + 1]
    ld_in[plane] = ldsend[plane]

    low_lanes = lax.broadcasted_iota(jnp.int32, (AB, 128), 1) < 64
    for i in range(TOK // AB):
        for p in range(NP):
            rows = slice(i * AB, (i + 1) * AB)
            ldx[rows, p * 128 : (p + 1) * 128] = jnp.where(
                low_lanes, ld[rows, 2 * p : 2 * p + 1], ld[rows, 2 * p + 1 : 2 * p + 2]
            )

    again_copy.wait()

    def norm_rows(i, _):
        pltpu.make_async_copy(
            tok_h.at[pl.ds(i * AB, AB)], tok.at[pl.ds(i * AB, AB)], tok_sem.at[i]
        ).wait()
        rows = pl.ds(pl.multiple_of(i * AB, AB), AB)
        x = tok[rows, :].astype(F32)
        mean_square = jnp.sum(x * x, axis=1, keepdims=True) * (1.0 / D)
        scale = lax.rsqrt(mean_square + norm_epsilon)
        normed[rows, :] = (tok[rows, :].astype(F32) * scale * again[...]).astype(BF16)
        return _

    lax.fori_loop(0, TOK // AB, norm_rows, 0)

    proj_copies[0].start()
    fgain_copy.start()
    outw_copy.start()
    exp_copy.start()
    down_copy.start()

    proj_copies[1].wait()
    ks[...] = dot(normed[...], proj[1]).astype(BF16)
    proj_copies[2].wait()
    vs[...] = dot(normed[...], proj[2]).astype(BF16)

    lanes32 = lax.broadcasted_iota(jnp.int32, (32, 128), 1) < 64
    for p in range(NP):
        cols = slice(p * 128, (p + 1) * 128)
        decay = jnp.exp(ldx[TOK - 1 : TOK, cols] - ldx[:, cols])
        scaled = (ks[:, cols].astype(F32) * decay).astype(BF16)
        m = lax.dot_general(
            scaled, vs[:, cols], (((0,), (0,)), ((), ())), preferred_element_type=F32
        )
        even = jnp.where(lanes32, m[0:32], pltpu.roll(m[32:64], 64, 1))
        odd = jnp.where(lanes32, pltpu.roll(m[64:96], 64, 1), m[96:128])
        ssend[2 * p] = even.astype(BF16)
        ssend[2 * p + 1] = odd.astype(BF16)

    s_in[plane] = ssend[plane]
    pl.semaphore_wait(barrier, PLANE - 1 + DEPTH - 1 + 3)
    for d in range(1, PLANE):
        j, dev = plane_peer(d)
        remote(ssend.at[j], s_in.at[plane], s_ss.at[d], s_rs.at[d], dev).start()
        remote(ldsend.at[j], ld_in.at[plane], ld_ss.at[d], ld_rs.at[d], dev).start()

    proj_copies[0].wait()
    qs[...] = (dot(normed[...], proj[0]) * 0.125).astype(BF16)

    def send_totals():
        for d in range(1, PLANE):
            remote(ldsend.at[0], ld_in.at[0], ld_ss.at[d], ld_rs.at[d], core_peer).wait_recv()
            remote(ssend.at[0], s_in.at[0], s_ss.at[d], s_rs.at[d], core_peer).wait_recv()
        passed = ld_in[0]
        for j in range(1, PLANE):
            passed = passed + ld_in[j]
        ltsend[...] = passed
        state = jnp.zeros((32, 128), F32)
        for j in range(PLANE):
            pref[j] = state
            state = jnp.exp(ld_in[j]) * state + s_in[j].astype(F32)
        tsend[...] = state.astype(BF16)
        for d in range(1, DEPTH):

            @pl.when(z + d < DEPTH)
            def _later(d=d):
                dev = ((z + d) * PLANE + plane, t)
                remote(tsend, t_in.at[z], t_ss.at[d], t_rs.at[d], dev).start()
                remote(ltsend, lt_in.at[z], lt_ss.at[d], lt_rs.at[d], dev).start()

    def send_prefixes():
        carry[...] = jnp.zeros((32, 128), F32)
        for j in range(DEPTH - 1):

            @pl.when(j < z)
            def _earlier(j=j):
                d = z - j
                remote(ltsend, lt_in.at[j], lt_ss.at[d], lt_rs.at[d], core_peer).wait_recv()
                remote(tsend, t_in.at[j], t_ss.at[d], t_rs.at[d], core_peer).wait_recv()
                carry[...] = jnp.exp(lt_in[j]) * carry[...] + t_in[j].astype(F32)

        state = carry[...]
        passed = jnp.zeros((1, 128), F32)
        for j in range(PLANE):
            isend[j] = (pref[j] + jnp.exp(passed) * state).astype(BF16)
            passed = passed + ld_in[j]
        i_in[plane] = isend[plane]
        for d in range(1, PLANE):
            j, dev = plane_peer(d)
            remote(isend.at[j], i_in.at[plane], i_ss.at[d], i_rs.at[d], dev).start()

    lanes512 = lax.broadcasted_iota(jnp.int32, (TOK, 128), 1) < 64
    causal = lax.broadcasted_iota(jnp.int32, (AB, AB), 0) >= lax.broadcasted_iota(
        jnp.int32, (AB, AB), 1
    )
    zero = jnp.zeros((), BF16)

    def pair_step(p, _):
        cols = pl.ds(pl.multiple_of(p * 128, 128), 128)
        kp = ks[:, cols]
        vp = vs[:, cols]
        for h in range(2):
            mine = lanes512 if h == 0 else jnp.logical_not(lanes512)
            vh = jnp.where(mine, vp.astype(F32), 0.0).astype(BF16)
            for i in range(TOK // AB):
                rows = slice(i * AB, (i + 1) * AB)
                span = (i + 1) * AB
                qh = jnp.where(mine[0:AB], qs[rows, cols].astype(F32), 0.0).astype(BF16)
                scores = lax.dot_general(
                    qh, kp[0:span], (((1,), (1,)), ((), ())), preferred_element_type=F32
                )
                here = ldx[rows, cols][:, 64 * h : 64 * h + 1]
                there = ldt[2 * p + h]
                parts = []
                for b in range(i + 1):
                    gap = here - there[:, b * AB : (b + 1) * AB]
                    if b == i:
                        gap = jnp.where(causal, gap, -1e30)
                    parts.append(
                        (scores[:, b * AB : (b + 1) * AB] * jnp.exp(gap)).astype(BF16)
                    )
                weights = parts[0] if i == 0 else jnp.concatenate(parts, axis=1)
                part = dot(weights, vh[0:span])
                if h == 0:
                    local[rows, cols] = part
                else:
                    local[rows, cols] = local[rows, cols] + part

        @pl.when(p == 1)
        def _totals():
            send_totals()

        @pl.when(p == 3)
        def _prefixes():
            send_prefixes()

        return _

    lax.fori_loop(0, NP, pair_step, 0)

    for d in range(1, PLANE):
        remote(isend.at[0], i_in.at[0], i_ss.at[d], i_rs.at[d], core_peer).wait_recv()
    for p in range(NP):
        even = i_in[2 * p].astype(F32)
        odd = i_in[2 * p + 1].astype(F32)
        inc[p, 0:32, :] = jnp.where(lanes32, even, 0.0).astype(BF16)
        inc[p, 32:64, :] = jnp.where(lanes32, pltpu.roll(even, 64, 1), 0.0).astype(BF16)
        inc[p, 64:96, :] = jnp.where(lanes32, 0.0, pltpu.roll(odd, 64, 1)).astype(BF16)
        inc[p, 96:128, :] = jnp.where(lanes32, 0.0, odd).astype(BF16)

    same_head = jnp.where(
        (lax.broadcasted_iota(jnp.int32, (128, 128), 0) < 64)
        == (lax.broadcasted_iota(jnp.int32, (128, 128), 1) < 64),
        1.0,
        0.0,
    ).astype(BF16)

    def partial_to_core(i):
        return remote(psend.at[i], prec.at[i], p_ss.at[i], p_rs.at[i], core_peer)

    def partial_to_chip(i):
        return remote(pisend.at[i], pirec.at[i], pi_ss.at[i], pi_rs.at[i], chip_peer)

    def stage_a(j):
        rows = pl.ds(pl.multiple_of(j * HG * RW, HG * RW), HG * RW)
        for p in range(NP):
            cols = slice(p * 128, (p + 1) * 128)
            carried = dot(qs[rows, cols], inc[p])
            attended = local[rows, cols] + carried * jnp.exp(ldx[rows, cols])
            square = attended * attended
            high = square.astype(BF16)
            low = (square - high.astype(F32)).astype(BF16)
            mean_square = (dot(high, same_head) + dot(low, same_head)) * (1.0 / 64)
            headed = (attended * lax.rsqrt(mean_square + head_epsilon)).astype(BF16)
            for g in range(HG):
                for kk in range(2):
                    core_slot = 1 - k if kk == 0 else k
                    for cc in range(2):
                        chip_slot = c if cc == 0 else 1 - c
                        at = pl.multiple_of(g * RW + core_slot * 2 * OW + chip_slot * OW, OW)
                        first = g * RW + (kk * 2 + cc) * OW
                        ho[pl.ds(at, OW), cols] = headed[first : first + OW]
        for n in range(4):
            cols = slice(n * 512, (n + 1) * 512)
            part = dot(ho[...], outw[:, cols])
            for g in range(HG):
                at = g * RW
                psend[j * HG + g, :, cols] = part[at : at + 2 * OW].astype(BF16)
                pk[j * HG + g, :, cols] = part[at + 2 * OW : at + 4 * OW]
        for g in range(HG):
            partial_to_core(j * HG + g).start()

    def stage_b(i):
        partial_to_core(i).wait_recv()
        pisend[i] = (pk[i, OW : 2 * OW, :] + prec[i, OW : 2 * OW, :].astype(F32)).astype(BF16)
        partial_to_chip(i).start()

    own_at = k * 2 * OW + c * OW

    def rows_to_core(i):
        return remote(
            xrows.at[i, pl.ds(2 * OW, OW)], xrows.at[i, pl.ds(0, OW)],
            xd_ss.at[i], xd_rs.at[i], core_peer,
        )

    def rows_to_ffn(i):
        return remote(
            xrows.at[i, pl.ds(2 * OW, OW)], xrows.at[i, pl.ds(3 * OW, OW)],
            xi_ss.at[i], xi_rs.at[i], ffn_peer,
        )

    def rows_forward(i):
        return remote(
            xrows.at[i, pl.ds(3 * OW, OW)], xrows.at[i, pl.ds(OW, OW)],
            xf_ss.at[i], xf_rs.at[i], core_peer,
        )

    def stage_c(i):
        partial_to_chip(i).wait_recv()
        rows = pl.ds(pl.multiple_of(i * RW + own_at, OW), OW)
        res = (
            tok[rows, :].astype(F32)
            + (pk[i, 0:OW, :] + prec[i, 0:OW, :].astype(F32) + pirec[i].astype(F32))
        ).astype(BF16)
        resid[i] = res
        wide = res.astype(F32)
        mean_square = jnp.sum(wide * wide, axis=1, keepdims=True) * (1.0 / D)
        scale = lax.rsqrt(mean_square + norm_epsilon)
        xrows[i, 2 * OW : 3 * OW, :] = (wide * scale * fgain[...]).astype(BF16)
        rows_to_ffn(i).start()
        rows_to_core(i).start()

    def stage_d(i):
        rows_to_ffn(i).wait_recv()
        rows_forward(i).start()

    def sums_to_core(i):
        return remote(ysend.at[i], yrec.at[i], y_ss.at[i], y_rs.at[i], core_peer)

    def sums_to_ffn(i):
        return remote(yisend.at[i], yirec.at[i], yi_ss.at[i], yi_rs.at[i], ffn_peer)

    def stage_x(j):
        for g in range(EG):
            rows_to_core(j * EG + g).wait_recv()
            rows_forward(j * EG + g).wait_recv()
        x = xrows[pl.ds(j * EG, EG)].reshape(EG * RW, D)
        for n in range(4):
            cols = slice(n * 256, (n + 1) * 256)
            gate = dot(x, wexp[0, :, cols])
            up = dot(x, wexp[1, :, cols])
            hidden[:, cols] = (gate / (1.0 + jnp.exp(-gate)) * up).astype(BF16)

    def stage_y(j):
        for n in range(4):
            cols = slice(n * 512, (n + 1) * 512)
            part = dot(hidden[...], wdown[:, cols])
            for g in range(EG):
                at = g * RW
                ysend[j * EG + g, :, cols] = part[at : at + 2 * OW].astype(BF16)
                yk[j * EG + g, :, cols] = part[at + 2 * OW : at + 4 * OW]
        for g in range(EG):
            sums_to_core(j * EG + g).start()

    def stage_f(i):
        sums_to_core(i).wait_recv()
        yisend[i] = (yk[i, OW : 2 * OW, :] + yrec[i, OW : 2 * OW, :].astype(F32)).astype(BF16)
        sums_to_ffn(i).start()

    own_rows = pl.ds(pl.multiple_of(own_at, OW), OW)
    chip_rows = pl.ds(pl.multiple_of(k * 2 * OW + (1 - c) * OW, OW), OW)

    def out_to_core(i):
        return remote(
            out.at[i, own_rows], out.at[i, own_rows], od_ss.at[i], od_rs.at[i], core_peer
        )

    def out_to_chip(i):
        return remote(
            out.at[i, own_rows], out.at[i, own_rows], oi_ss.at[i], oi_rs.at[i], chip_peer
        )

    def out_forward(i):
        return remote(
            out.at[i, chip_rows], out.at[i, chip_rows], of_ss.at[i], of_rs.at[i], core_peer
        )

    def stage_g(i):
        sums_to_ffn(i).wait_recv()
        out[i, own_rows, :] = (
            resid[i].astype(F32)
            + (yk[i, 0:OW, :] + yrec[i, 0:OW, :].astype(F32) + yirec[i].astype(F32))
        ).astype(BF16)
        out_to_chip(i).start()
        out_to_core(i).start()

    def stage_h(i):
        out_to_chip(i).wait_recv()
        out_forward(i).start()

    def stage_z(i):
        out_to_core(i).wait_recv()
        out_forward(i).wait_recv()

    outw_copy.wait()
    fgain_copy.wait()
    stages = {
        "A": stage_a, "B": stage_b, "C": stage_c, "D": stage_d, "X": stage_x,
        "Y": stage_y, "F": stage_f, "G": stage_g, "H": stage_h, "Z": stage_z,
    }
    ops = [(word[0], int(word[1:])) for part in ORDER for word in part.split()]

    def run(some):
        for name, i in some:
            stages[name](i)

    def between(first, last):
        start = ops.index(first) + 1
        return ops[start : ops.index(last)] if last in ops else ops[start:]

    def guarded(step, lists):
        for i, some in enumerate(lists):
            if some:
                pl.when(step == i)(functools.partial(run, some))

    groups = CH // HG
    after_a = [between(("A", j), ("A", j + 1)) for j in range(groups - 1)]
    middle = between(("A", groups - 1), ("X", 0))
    steps = CH // EG
    inside = [between(("X", j), ("Y", j)) for j in range(steps)]
    after_y = [between(("Y", j), ("X", j + 1)) for j in range(steps - 1)]
    tail = between(("Y", steps - 1), None)

    def heads_step(i, _):
        stage_a(i)
        guarded(i, after_a)
        return _

    lax.fori_loop(0, groups, heads_step, 0)
    run(middle)
    exp_copy.wait()
    down_copy.wait()

    def ffn_step(j, _):
        stage_x(j)
        guarded(j, inside)
        stage_y(j)
        guarded(j, after_y)
        return _

    lax.fori_loop(0, steps, ffn_step, 0)
    run(tail)

    for d in range(1, PLANE):
        remote(ldsend.at[0], ld_in.at[0], ld_ss.at[d], ld_rs.at[d], core_peer).wait_send()
        remote(ssend.at[0], s_in.at[0], s_ss.at[d], s_rs.at[d], core_peer).wait_send()
        remote(isend.at[0], i_in.at[0], i_ss.at[d], i_rs.at[d], core_peer).wait_send()
    for d in range(1, DEPTH):

        @pl.when(z + d < DEPTH)
        def _sent(d=d):
            remote(ltsend, lt_in.at[0], lt_ss.at[d], lt_rs.at[d], core_peer).wait_send()
            remote(tsend, t_in.at[0], t_ss.at[d], t_rs.at[d], core_peer).wait_send()

    for i in range(CH):
        for copy in (
            partial_to_core, partial_to_chip, rows_to_core, rows_to_ffn, rows_forward,
            sums_to_core, sums_to_ffn, out_to_core, out_to_chip, out_forward,
        ):
            copy(i).wait_send()


def local_layer(tokens, forget, attn_gain, projections, out_weight, ffn_gain, expand_weight, down_weight):
    dma = pltpu.SemaphoreType.DMA
    vmem = pltpu.VMEM
    scratch = [
        vmem((TOK, D), BF16),
        vmem((8, TOK), F32),
        vmem((1, D), F32),
        vmem((1, D), F32),
        vmem((3, D, HD), BF16),
        vmem((HD, D), BF16),
        vmem((2, D, FF), BF16),
        vmem((FF, D), BF16),
        vmem((TOK, D), BF16),
        vmem((TOK, HD), BF16),
        vmem((TOK, HD), BF16),
        vmem((TOK, HD), BF16),
        vmem((TOK, 128), F32),
        vmem((8, 1, TOK), F32),
        vmem((TOK, HD), F32),
        vmem((TOK, HD), F32),
        vmem((PLANE, 1, 128), F32),
        vmem((PLANE, 1, 128), F32),
        vmem((1, 128), F32),
        vmem((DEPTH, 1, 128), F32),
        vmem((PLANE, 32, 128), BF16),
        vmem((PLANE, 32, 128), BF16),
        vmem((PLANE, 32, 128), F32),
        vmem((32, 128), F32),
        vmem((32, 128), BF16),
        vmem((DEPTH, 32, 128), BF16),
        vmem((PLANE, 32, 128), BF16),
        vmem((PLANE, 32, 128), BF16),
        vmem((NP, 128, 128), BF16),
        vmem((HG * RW, HD), BF16),
        vmem((CH, 2 * OW, D), BF16),
        vmem((CH, 2 * OW, D), BF16),
        vmem((CH, 2 * OW, D), F32),
        vmem((CH, OW, D), BF16),
        vmem((CH, OW, D), BF16),
        vmem((CH, OW, D), BF16),
        vmem((CH, RW, D), BF16),
        vmem((EG * RW, FF), BF16),
        vmem((CH, 2 * OW, D), BF16),
        vmem((CH, 2 * OW, D), BF16),
        vmem((CH, 2 * OW, D), F32),
        vmem((CH, OW, D), BF16),
        vmem((CH, OW, D), BF16),
        dma((TOK // AB,)),
        dma((9,)),
    ]
    scratch += [dma((8,)) for _ in range(10)]
    scratch += [dma((CH,)) for _ in range(20)]
    any_spec = pl.BlockSpec(memory_space=pl.ANY)
    result = pl.pallas_call(
        kernel,
        out_shape=vmem((CH, RW, D), BF16),
        in_specs=[any_spec] * 8,
        out_specs=pl.BlockSpec(memory_space=vmem),
        scratch_shapes=scratch,
        name="layer",
        compiler_params=pltpu.CompilerParams(
            collective_id=0, has_side_effects=True, vmem_limit_bytes=58 * 1024 * 1024
        ),
    )(
        tokens,
        forget.T,
        attn_gain.reshape(1, D),
        projections,
        out_weight,
        ffn_gain.reshape(1, D),
        expand_weight,
        down_weight,
    )
    return result.reshape(TOK, D)


def solution(mesh):
    return jax.shard_map(
        local_layer,
        mesh=mesh,
        in_specs=(
            P("seq", None),
            P("seq", "tp"),
            P(),
            P(None, None, "tp"),
            P("tp", None),
            P(),
            P(None, None, "tp"),
            P("tp", None),
        ),
        out_specs=P("seq", None),
        check_vma=False,
    )
```

```python
import functools

import jax
import jax.numpy as jnp
from jax import lax
from jax.experimental import pallas as pl
from jax.experimental.pallas import tpu as pltpu
from jax.sharding import PartitionSpec as P

MESH = pl.DeviceIdType.MESH
F32 = jnp.float32
BF16 = jnp.bfloat16

norm_epsilon = 1e-05
head_epsilon = 1e-06

TOK = 512
D = 2048
HD = 512
FF = 1024
CH = 8
EG = 2
HG = 2
AB = 128
RW = TOK // CH
OW = RW // 4
NP = 4
PLANE = 8
DEPTH = 8
FAR_FIRST = (4, 3, 5, 2, 6, 1, 7)


ORDER = (
    "A0 A1 B0 B1", "B2 B3 A2 A3", "B5 C0 B4 B6", "C1 C2 C3 B7", "D0 C5 D1 C4", "D2 C6 X0 D3",
    "C7 Y0 D5 X1", "D4 F1 F0 Y1", "D6 X2 D7 F2", "F3 Y2 X3 F4", "G1 Y3 G0 F5", "F6 G2 F7 G3",
    "H1 G4 G5 G6", "G7 H2 H4 H5", "H3 Z4 H6 H0", "H7 Z1 Z3 Z5", "Z7 Z0 Z2 Z6",
)


def dot(a, b):
    return jnp.dot(a, b, preferred_element_type=F32)


def kernel(
    tok_h, forget_h, again_h, proj_h, outw_h, fgain_h, exp_h, down_h, out,
    tok, fgt, again, fgain, proj, outw, wexp, wdown,
    normed, qs, ks, vs, ld, ldt, ldx, local,
    ldsend, ld_in, ltsend, lt_in, ssend, s_in, pref, carry, tsend, t_in, isend, i_in, inc,
    ho, psend, prec, pk, pisend, pirec,
    resid, xrows, hidden, ysend, yrec, yk, yisend, yirec,
    tok_sem, w_sem,
    ld_ss, ld_rs, lt_ss, lt_rs, s_ss, s_rs, t_ss, t_rs, i_ss, i_rs,
    p_ss, p_rs, pi_ss, pi_rs, xd_ss, xd_rs, xi_ss, xi_rs, xf_ss, xf_rs,
    y_ss, y_rs, yi_ss, yi_rs, od_ss, od_rs, oi_ss, oi_rs, of_ss, of_rs,
):
    s = lax.axis_index("seq")
    t = lax.axis_index("tp")
    plane = lax.rem(s, PLANE)
    z = s // PLANE
    c = t // 2
    k = lax.rem(t, 2)
    core_peer = (s, c * 2 + (1 - k))
    chip_peer = (s, (1 - c) * 2 + k)
    ffn_peer = (s + 1 - 2 * lax.rem(s, 2), (1 - c) * 2 + k)

    def plane_peer(d):
        j = lax.rem(plane + d, PLANE)
        return j, (z * PLANE + j, t)

    def depth_peer(d):
        j = lax.rem(z + d, DEPTH)
        return j, (j * PLANE + plane, t)

    def remote(src, dst, ssem, rsem, dev):
        return pltpu.make_async_remote_copy(
            src_ref=src, dst_ref=dst, send_sem=ssem, recv_sem=rsem,
            device_id=dev, device_id_type=MESH,
        )

    barrier = pltpu.get_barrier_semaphore()
    for d in range(1, PLANE):
        pl.semaphore_signal(barrier, inc=1, device_id=plane_peer(d)[1], device_id_type=MESH)
    for d in range(1, DEPTH):
        pl.semaphore_signal(barrier, inc=1, device_id=depth_peer(d)[1], device_id_type=MESH)
    for dev in (core_peer, chip_peer, ffn_peer):
        pl.semaphore_signal(barrier, inc=1, device_id=dev, device_id_type=MESH)

    for i in range(TOK // AB):
        rows = pl.ds(i * AB, AB)
        pltpu.make_async_copy(tok_h.at[rows], tok.at[rows], tok_sem.at[i]).start()
    forget_copy = pltpu.make_async_copy(forget_h, fgt, w_sem.at[0])
    again_copy = pltpu.make_async_copy(again_h, again, w_sem.at[1])
    proj_copies = [
        pltpu.make_async_copy(proj_h.at[w], proj.at[w], w_sem.at[2 + w]) for w in range(3)
    ]
    fgain_copy = pltpu.make_async_copy(fgain_h, fgain, w_sem.at[5])
    outw_copy = pltpu.make_async_copy(outw_h, outw, w_sem.at[6])
    exp_copy = pltpu.make_async_copy(exp_h, wexp, w_sem.at[7])
    down_copy = pltpu.make_async_copy(down_h, wdown, w_sem.at[8])
    forget_copy.start()
    again_copy.start()
    proj_copies[1].start()
    proj_copies[2].start()

    forget_copy.wait()
    f = fgt[...]
    f1 = f.astype(BF16)
    rest = f - f1.astype(F32)
    f2 = rest.astype(BF16)
    f3 = (rest - f2.astype(F32)).astype(BF16)
    row_at = lax.broadcasted_iota(jnp.int32, (TOK, TOK), 0)
    col_at = lax.broadcasted_iota(jnp.int32, (TOK, TOK), 1)
    upper = jnp.where(row_at <= col_at, 1.0, 0.0).astype(BF16)
    turned = dot(f1, upper) + (dot(f2, upper) + dot(f3, upper))
    for h in range(8):
        ldt[h] = turned[h : h + 1]
    ld[...] = jnp.transpose(jnp.concatenate([turned, jnp.zeros((120, TOK), F32)], axis=0))
    total = jnp.broadcast_to(turned[:, TOK - 1 : TOK], (8, 128))
    for h in range(8):
        ldsend[h] = total[h : h + 1]
    ld_in[plane] = ldsend[plane]

    low_lanes = lax.broadcasted_iota(jnp.int32, (AB, 128), 1) < 64
    for i in range(TOK // AB):
        for p in range(NP):
            rows = slice(i * AB, (i + 1) * AB)
            ldx[rows, p * 128 : (p + 1) * 128] = jnp.where(
                low_lanes, ld[rows, 2 * p : 2 * p + 1], ld[rows, 2 * p + 1 : 2 * p + 2]
            )

    again_copy.wait()

    def norm_rows(i, _):
        pltpu.make_async_copy(
            tok_h.at[pl.ds(i * AB, AB)], tok.at[pl.ds(i * AB, AB)], tok_sem.at[i]
        ).wait()
        rows = pl.ds(pl.multiple_of(i * AB, AB), AB)
        x = tok[rows, :].astype(F32)
        mean_square = jnp.sum(x * x, axis=1, keepdims=True) * (1.0 / D)
        scale = lax.rsqrt(mean_square + norm_epsilon)
        normed[rows, :] = (tok[rows, :].astype(F32) * scale * again[...]).astype(BF16)
        return _

    lax.fori_loop(0, TOK // AB, norm_rows, 0)

    proj_copies[0].start()
    fgain_copy.start()
    outw_copy.start()
    exp_copy.start()
    down_copy.start()

    proj_copies[1].wait()
    ks[...] = dot(normed[...], proj[1]).astype(BF16)
    proj_copies[2].wait()
    vs[...] = dot(normed[...], proj[2]).astype(BF16)

    lanes32 = lax.broadcasted_iota(jnp.int32, (32, 128), 1) < 64
    for p in range(NP):
        cols = slice(p * 128, (p + 1) * 128)
        decay = jnp.exp(ldx[TOK - 1 : TOK, cols] - ldx[:, cols])
        scaled = (ks[:, cols].astype(F32) * decay).astype(BF16)
        m = lax.dot_general(
            scaled, vs[:, cols], (((0,), (0,)), ((), ())), preferred_element_type=F32
        )
        even = jnp.where(lanes32, m[0:32], pltpu.roll(m[32:64], 64, 1))
        odd = jnp.where(lanes32, pltpu.roll(m[64:96], 64, 1), m[96:128])
        ssend[2 * p] = even.astype(BF16)
        ssend[2 * p + 1] = odd.astype(BF16)

    s_in[plane] = ssend[plane]
    pl.semaphore_wait(barrier, PLANE - 1 + DEPTH - 1 + 3)
    for d in FAR_FIRST:
        j, dev = plane_peer(d)
        remote(ssend.at[j], s_in.at[plane], s_ss.at[d], s_rs.at[d], dev).start()
    for d in FAR_FIRST:
        j, dev = plane_peer(d)
        remote(ldsend.at[j], ld_in.at[plane], ld_ss.at[d], ld_rs.at[d], dev).start()

    proj_copies[0].wait()
    qs[...] = (dot(normed[...], proj[0]) * 0.125).astype(BF16)

    def send_totals():
        for d in range(1, PLANE):
            remote(ldsend.at[0], ld_in.at[0], ld_ss.at[d], ld_rs.at[d], core_peer).wait_recv()
            remote(ssend.at[0], s_in.at[0], s_ss.at[d], s_rs.at[d], core_peer).wait_recv()
        passed = ld_in[0]
        for j in range(1, PLANE):
            passed = passed + ld_in[j]
        ltsend[...] = passed
        state = jnp.zeros((32, 128), F32)
        for j in range(PLANE):
            pref[j] = state
            state = jnp.exp(ld_in[j]) * state + s_in[j].astype(F32)
        tsend[...] = state.astype(BF16)
        for d in FAR_FIRST:

            @pl.when(z + d < DEPTH)
            def _later(d=d):
                dev = ((z + d) * PLANE + plane, t)
                remote(tsend, t_in.at[z], t_ss.at[d], t_rs.at[d], dev).start()
                remote(ltsend, lt_in.at[z], lt_ss.at[d], lt_rs.at[d], dev).start()

    def send_prefixes():
        carry[...] = jnp.zeros((32, 128), F32)
        for j in range(DEPTH - 1):

            @pl.when(j < z)
            def _earlier(j=j):
                d = z - j
                remote(ltsend, lt_in.at[j], lt_ss.at[d], lt_rs.at[d], core_peer).wait_recv()
                remote(tsend, t_in.at[j], t_ss.at[d], t_rs.at[d], core_peer).wait_recv()
                carry[...] = jnp.exp(lt_in[j]) * carry[...] + t_in[j].astype(F32)

        state = carry[...]
        passed = jnp.zeros((1, 128), F32)
        for j in range(PLANE):
            isend[j] = (pref[j] + jnp.exp(passed) * state).astype(BF16)
            passed = passed + ld_in[j]
        i_in[plane] = isend[plane]
        for d in FAR_FIRST:
            j, dev = plane_peer(d)
            remote(isend.at[j], i_in.at[plane], i_ss.at[d], i_rs.at[d], dev).start()

    lanes512 = lax.broadcasted_iota(jnp.int32, (TOK, 128), 1) < 64
    causal = lax.broadcasted_iota(jnp.int32, (AB, AB), 0) >= lax.broadcasted_iota(
        jnp.int32, (AB, AB), 1
    )
    zero = jnp.zeros((), BF16)

    def pair_step(p, _):
        cols = pl.ds(pl.multiple_of(p * 128, 128), 128)
        kp = ks[:, cols]
        vp = vs[:, cols]
        for h in range(2):
            mine = lanes512 if h == 0 else jnp.logical_not(lanes512)
            vh = jnp.where(mine, vp.astype(F32), 0.0).astype(BF16)
            for i in range(TOK // AB):
                rows = slice(i * AB, (i + 1) * AB)
                span = (i + 1) * AB
                qh = jnp.where(mine[0:AB], qs[rows, cols].astype(F32), 0.0).astype(BF16)
                scores = lax.dot_general(
                    qh, kp[0:span], (((1,), (1,)), ((), ())), preferred_element_type=F32
                )
                here = ldx[rows, cols][:, 64 * h : 64 * h + 1]
                there = ldt[2 * p + h]
                parts = []
                for b in range(i + 1):
                    gap = here - there[:, b * AB : (b + 1) * AB]
                    if b == i:
                        gap = jnp.where(causal, gap, -1e30)
                    parts.append(
                        (scores[:, b * AB : (b + 1) * AB] * jnp.exp(gap)).astype(BF16)
                    )
                weights = parts[0] if i == 0 else jnp.concatenate(parts, axis=1)
                part = dot(weights, vh[0:span])
                if h == 0:
                    local[rows, cols] = part
                else:
                    local[rows, cols] = local[rows, cols] + part

        @pl.when(p == 1)
        def _totals():
            send_totals()

        @pl.when(p == 3)
        def _prefixes():
            send_prefixes()

        return _

    lax.fori_loop(0, NP, pair_step, 0)

    for d in range(1, PLANE):
        remote(isend.at[0], i_in.at[0], i_ss.at[d], i_rs.at[d], core_peer).wait_recv()
    for p in range(NP):
        even = i_in[2 * p].astype(F32)
        odd = i_in[2 * p + 1].astype(F32)
        inc[p, 0:32, :] = jnp.where(lanes32, even, 0.0).astype(BF16)
        inc[p, 32:64, :] = jnp.where(lanes32, pltpu.roll(even, 64, 1), 0.0).astype(BF16)
        inc[p, 64:96, :] = jnp.where(lanes32, 0.0, pltpu.roll(odd, 64, 1)).astype(BF16)
        inc[p, 96:128, :] = jnp.where(lanes32, 0.0, odd).astype(BF16)

    same_head = jnp.where(
        (lax.broadcasted_iota(jnp.int32, (128, 128), 0) < 64)
        == (lax.broadcasted_iota(jnp.int32, (128, 128), 1) < 64),
        1.0,
        0.0,
    ).astype(BF16)

    def partial_to_core(i):
        return remote(psend.at[i], prec.at[i], p_ss.at[i], p_rs.at[i], core_peer)

    def partial_to_chip(i):
        return remote(pisend.at[i], pirec.at[i], pi_ss.at[i], pi_rs.at[i], chip_peer)

    def stage_a(j):
        rows = pl.ds(pl.multiple_of(j * HG * RW, HG * RW), HG * RW)
        for p in range(NP):
            cols = slice(p * 128, (p + 1) * 128)
            carried = dot(qs[rows, cols], inc[p])
            attended = local[rows, cols] + carried * jnp.exp(ldx[rows, cols])
            square = attended * attended
            high = square.astype(BF16)
            low = (square - high.astype(F32)).astype(BF16)
            mean_square = (dot(high, same_head) + dot(low, same_head)) * (1.0 / 64)
            headed = (attended * lax.rsqrt(mean_square + head_epsilon)).astype(BF16)
            for g in range(HG):
                for kk in range(2):
                    core_slot = 1 - k if kk == 0 else k
                    for cc in range(2):
                        chip_slot = c if cc == 0 else 1 - c
                        at = pl.multiple_of(g * RW + core_slot * 2 * OW + chip_slot * OW, OW)
                        first = g * RW + (kk * 2 + cc) * OW
                        ho[pl.ds(at, OW), cols] = headed[first : first + OW]
        for n in range(4):
            cols = slice(n * 512, (n + 1) * 512)
            part = dot(ho[...], outw[:, cols])
            for g in range(HG):
                at = g * RW
                psend[j * HG + g, :, cols] = part[at : at + 2 * OW].astype(BF16)
                pk[j * HG + g, :, cols] = part[at + 2 * OW : at + 4 * OW]
        for g in range(HG):
            partial_to_core(j * HG + g).start()

    def stage_b(i):
        partial_to_core(i).wait_recv()
        pisend[i] = (pk[i, OW : 2 * OW, :] + prec[i, OW : 2 * OW, :].astype(F32)).astype(BF16)
        partial_to_chip(i).start()

    own_at = k * 2 * OW + c * OW

    def rows_to_core(i):
        return remote(
            xrows.at[i, pl.ds(2 * OW, OW)], xrows.at[i, pl.ds(0, OW)],
            xd_ss.at[i], xd_rs.at[i], core_peer,
        )

    def rows_to_ffn(i):
        return remote(
            xrows.at[i, pl.ds(2 * OW, OW)], xrows.at[i, pl.ds(3 * OW, OW)],
            xi_ss.at[i], xi_rs.at[i], ffn_peer,
        )

    def rows_forward(i):
        return remote(
            xrows.at[i, pl.ds(3 * OW, OW)], xrows.at[i, pl.ds(OW, OW)],
            xf_ss.at[i], xf_rs.at[i], core_peer,
        )

    def stage_c(i):
        partial_to_chip(i).wait_recv()
        rows = pl.ds(pl.multiple_of(i * RW + own_at, OW), OW)
        res = (
            tok[rows, :].astype(F32)
            + (pk[i, 0:OW, :] + prec[i, 0:OW, :].astype(F32) + pirec[i].astype(F32))
        ).astype(BF16)
        resid[i] = res
        wide = res.astype(F32)
        mean_square = jnp.sum(wide * wide, axis=1, keepdims=True) * (1.0 / D)
        scale = lax.rsqrt(mean_square + norm_epsilon)
        xrows[i, 2 * OW : 3 * OW, :] = (wide * scale * fgain[...]).astype(BF16)
        rows_to_ffn(i).start()
        rows_to_core(i).start()

    def stage_d(i):
        rows_to_ffn(i).wait_recv()
        rows_forward(i).start()

    def sums_to_core(i):
        return remote(ysend.at[i], yrec.at[i], y_ss.at[i], y_rs.at[i], core_peer)

    def sums_to_ffn(i):
        return remote(yisend.at[i], yirec.at[i], yi_ss.at[i], yi_rs.at[i], ffn_peer)

    def stage_x(j):
        for g in range(EG):
            rows_to_core(j * EG + g).wait_recv()
            rows_forward(j * EG + g).wait_recv()
        x = xrows[pl.ds(j * EG, EG)].reshape(EG * RW, D)
        for n in range(4):
            cols = slice(n * 256, (n + 1) * 256)
            gate = dot(x, wexp[0, :, cols])
            up = dot(x, wexp[1, :, cols])
            hidden[:, cols] = (gate / (1.0 + jnp.exp(-gate)) * up).astype(BF16)

    def stage_y(j):
        for n in range(4):
            cols = slice(n * 512, (n + 1) * 512)
            part = dot(hidden[...], wdown[:, cols])
            for g in range(EG):
                at = g * RW
                ysend[j * EG + g, :, cols] = part[at : at + 2 * OW].astype(BF16)
                yk[j * EG + g, :, cols] = part[at + 2 * OW : at + 4 * OW]
        for g in range(EG):
            sums_to_core(j * EG + g).start()

    def stage_f(i):
        sums_to_core(i).wait_recv()
        yisend[i] = (yk[i, OW : 2 * OW, :] + yrec[i, OW : 2 * OW, :].astype(F32)).astype(BF16)
        sums_to_ffn(i).start()

    own_rows = pl.ds(pl.multiple_of(own_at, OW), OW)
    chip_rows = pl.ds(pl.multiple_of(k * 2 * OW + (1 - c) * OW, OW), OW)

    def out_to_core(i):
        return remote(
            out.at[i, own_rows], out.at[i, own_rows], od_ss.at[i], od_rs.at[i], core_peer
        )

    def out_to_chip(i):
        return remote(
            out.at[i, own_rows], out.at[i, own_rows], oi_ss.at[i], oi_rs.at[i], chip_peer
        )

    def out_forward(i):
        return remote(
            out.at[i, chip_rows], out.at[i, chip_rows], of_ss.at[i], of_rs.at[i], core_peer
        )

    def stage_g(i):
        sums_to_ffn(i).wait_recv()
        out[i, own_rows, :] = (
            resid[i].astype(F32)
            + (yk[i, 0:OW, :] + yrec[i, 0:OW, :].astype(F32) + yirec[i].astype(F32))
        ).astype(BF16)
        out_to_chip(i).start()
        out_to_core(i).start()

    def stage_h(i):
        out_to_chip(i).wait_recv()
        out_forward(i).start()

    def stage_z(i):
        out_to_core(i).wait_recv()
        out_forward(i).wait_recv()

    outw_copy.wait()
    fgain_copy.wait()
    stages = {
        "A": stage_a, "B": stage_b, "C": stage_c, "D": stage_d, "X": stage_x,
        "Y": stage_y, "F": stage_f, "G": stage_g, "H": stage_h, "Z": stage_z,
    }
    ops = [(word[0], int(word[1:])) for part in ORDER for word in part.split()]

    def run(some):
        for name, i in some:
            stages[name](i)

    def between(first, last):
        start = ops.index(first) + 1
        return ops[start : ops.index(last)] if last in ops else ops[start:]

    def guarded(step, lists):
        for i, some in enumerate(lists):
            if some:
                pl.when(step == i)(functools.partial(run, some))

    groups = CH // HG
    after_a = [between(("A", j), ("A", j + 1)) for j in range(groups - 1)]
    middle = between(("A", groups - 1), ("X", 0))
    steps = CH // EG
    inside = [between(("X", j), ("Y", j)) for j in range(steps)]
    after_y = [between(("Y", j), ("X", j + 1)) for j in range(steps - 1)]
    tail = between(("Y", steps - 1), None)

    def heads_step(i, _):
        stage_a(i)
        guarded(i, after_a)
        return _

    lax.fori_loop(0, groups, heads_step, 0)
    run(middle)
    exp_copy.wait()
    down_copy.wait()

    def ffn_step(j, _):
        stage_x(j)
        guarded(j, inside)
        stage_y(j)
        guarded(j, after_y)
        return _

    lax.fori_loop(0, steps, ffn_step, 0)
    run(tail)

    for d in range(1, PLANE):
        remote(ldsend.at[0], ld_in.at[0], ld_ss.at[d], ld_rs.at[d], core_peer).wait_send()
        remote(ssend.at[0], s_in.at[0], s_ss.at[d], s_rs.at[d], core_peer).wait_send()
        remote(isend.at[0], i_in.at[0], i_ss.at[d], i_rs.at[d], core_peer).wait_send()
    for d in range(1, DEPTH):

        @pl.when(z + d < DEPTH)
        def _sent(d=d):
            remote(ltsend, lt_in.at[0], lt_ss.at[d], lt_rs.at[d], core_peer).wait_send()
            remote(tsend, t_in.at[0], t_ss.at[d], t_rs.at[d], core_peer).wait_send()

    for i in range(CH):
        for copy in (
            partial_to_core, partial_to_chip, rows_to_core, rows_to_ffn, rows_forward,
            sums_to_core, sums_to_ffn, out_to_core, out_to_chip, out_forward,
        ):
            copy(i).wait_send()


def local_layer(tokens, forget, attn_gain, projections, out_weight, ffn_gain, expand_weight, down_weight):
    dma = pltpu.SemaphoreType.DMA
    vmem = pltpu.VMEM
    scratch = [
        vmem((TOK, D), BF16),
        vmem((8, TOK), F32),
        vmem((1, D), F32),
        vmem((1, D), F32),
        vmem((3, D, HD), BF16),
        vmem((HD, D), BF16),
        vmem((2, D, FF), BF16),
        vmem((FF, D), BF16),
        vmem((TOK, D), BF16),
        vmem((TOK, HD), BF16),
        vmem((TOK, HD), BF16),
        vmem((TOK, HD), BF16),
        vmem((TOK, 128), F32),
        vmem((8, 1, TOK), F32),
        vmem((TOK, HD), F32),
        vmem((TOK, HD), F32),
        vmem((PLANE, 1, 128), F32),
        vmem((PLANE, 1, 128), F32),
        vmem((1, 128), F32),
        vmem((DEPTH, 1, 128), F32),
        vmem((PLANE, 32, 128), BF16),
        vmem((PLANE, 32, 128), BF16),
        vmem((PLANE, 32, 128), F32),
        vmem((32, 128), F32),
        vmem((32, 128), BF16),
        vmem((DEPTH, 32, 128), BF16),
        vmem((PLANE, 32, 128), BF16),
        vmem((PLANE, 32, 128), BF16),
        vmem((NP, 128, 128), BF16),
        vmem((HG * RW, HD), BF16),
        vmem((CH, 2 * OW, D), BF16),
        vmem((CH, 2 * OW, D), BF16),
        vmem((CH, 2 * OW, D), F32),
        vmem((CH, OW, D), BF16),
        vmem((CH, OW, D), BF16),
        vmem((CH, OW, D), BF16),
        vmem((CH, RW, D), BF16),
        vmem((EG * RW, FF), BF16),
        vmem((CH, 2 * OW, D), BF16),
        vmem((CH, 2 * OW, D), BF16),
        vmem((CH, 2 * OW, D), F32),
        vmem((CH, OW, D), BF16),
        vmem((CH, OW, D), BF16),
        dma((TOK // AB,)),
        dma((9,)),
    ]
    scratch += [dma((8,)) for _ in range(10)]
    scratch += [dma((CH,)) for _ in range(20)]
    any_spec = pl.BlockSpec(memory_space=pl.ANY)
    result = pl.pallas_call(
        kernel,
        out_shape=vmem((CH, RW, D), BF16),
        in_specs=[any_spec] * 8,
        out_specs=pl.BlockSpec(memory_space=vmem),
        scratch_shapes=scratch,
        name="layer",
        compiler_params=pltpu.CompilerParams(
            collective_id=0, has_side_effects=True, vmem_limit_bytes=58 * 1024 * 1024
        ),
    )(
        tokens,
        forget.T,
        attn_gain.reshape(1, D),
        projections,
        out_weight,
        ffn_gain.reshape(1, D),
        expand_weight,
        down_weight,
    )
    return result.reshape(TOK, D)


def solution(mesh):
    return jax.shard_map(
        local_layer,
        mesh=mesh,
        in_specs=(
            P("seq", None),
            P("seq", "tp"),
            P(),
            P(None, None, "tp"),
            P("tp", None),
            P(),
            P(None, None, "tp"),
            P("tp", None),
        ),
        out_specs=P("seq", None),
        check_vma=False,
    )
```
